256 devices in a mesh: gx: 16 (over z, x_lo), gy: 16 (over y, x_hi, core).
Axes of the slice: x: 4 (x_hi: 2, x_lo: 2; x = x_hi * 2 + x_lo), y: 4, z: 8, core: 2. Of those that a mesh axis runs over, the one named last changes fastest.
Arguments:
- gradient: float32 [2048, 512], P('gx', 'gy'), may hold values from -6 to 6
- stat_old: float32 [2048, 2048], P('gx', 'gy'), may hold values from -1.001 to 1.001, as said below
Outputs:
- statistic: float32 [2048, 2048], P('gx', 'gy')
- inverse_root: float32 [2048, 2048], P('gx', 'gy')
The draws below stay inside these ranges and needn't reach their ends.
Inputs may be any that keep to these rules, and one draw needn't show every extreme that they name: stat_old is symmetric positive semidefinite with unit diagonal, the Gram matrix of 2048 unit-length rows of 512 entries.
All inputs are finite; a program needn't handle non-finite values.
Results may differ from the reference program's by a relative error of at most 0.0003.
Values sent between devices are 32-bit elements.
No kernel may reach another device: no remote copies, remote signals or barrier semaphores. Data moves between devices by JAX's collectives and lax.ppermute only.
A program may use at most 64 MiB of HBM per device.

```python
import jax
import jax.numpy as jnp
from jax import lax

NSIDE = 2048
MCOLS = 512


def draw_stat_old(key, part):
    factor = jax.random.normal(key, (NSIDE, NSIDE // 4), jnp.float32)
    lengths = jnp.sqrt(jnp.sum(factor * factor, axis=1, keepdims=True))
    factor = factor / lengths
    return jnp.dot(factor, factor.T, preferred_element_type=jnp.float32, precision=lax.Precision.HIGHEST)


def steps_of(stream_key, dims, pieces, low, high):
    factor_of = 1.0
    for dim, shards_of in pieces:
        draws = jax.random.uniform(jax.random.fold_in(jax.random.fold_in(stream_key, 6), dim), (shards_of,), jnp.float32, low / len(pieces), high / len(pieces))
        factor_of = factor_of * jnp.repeat(jnp.exp(draws), dims[dim] // shards_of).reshape((-1,) + (1,) * (len(dims) - 1 - dim))
    return factor_of


def bell_draw(rng, dims, width, reach, pieces=(), kind=jnp.bfloat16):
    array = jax.random.normal(rng, dims, jnp.float32) * width
    if len(pieces) > 0:
        array = steps_of(rng, dims, pieces, -0.22, 0.18) * array
    return jnp.clip(array, min=-reach, max=reach).astype(kind)


def setup_inputs(seed: int = 0) -> dict:
    key_of = jax.random.split(jax.random.key(seed), 3)
    return {
        "gradient": bell_draw(key_of[0], (NSIDE, MCOLS), 1.0, 6.0, ((0, 16), (1, 16)), jnp.float32),
        "stat_old": draw_stat_old(jax.random.fold_in(key_of[2], 71), 0),
    }


def matmul(leading, trailing):
    return jnp.dot(leading, trailing, preferred_element_type=jnp.float32, precision=lax.Precision.HIGHEST)

def reference(gradient, stat_old):
    statistic = 0.9 * stat_old + matmul(gradient, gradient.T) / MCOLS
    divisor = 2.0 * jnp.sqrt(jnp.sum(statistic * statistic) / NSIDE)
    identity = jnp.eye(NSIDE, dtype=jnp.float32)
    normed = statistic / divisor
    first_step = 1.5 * identity - 0.5 * normed
    root_half = matmul(normed, first_step)
    product_mid = matmul(first_step, root_half)
    second_step = 1.5 * identity - 0.5 * product_mid
    inverse_root = matmul(second_step, first_step)
    return (statistic, inverse_root)
```

```python
import jax
import jax.numpy as jnp
from jax import lax
from jax.sharding import Mesh
from jax.sharding import PartitionSpec as P

Z, XL, Y, XH, CORE = "gx_0", "gx_1", "gy_0", "gy_1", "gy_2"
GX = (Z, XL)
GY = (Y, XH, CORE)


def matmul(leading, trailing):
    return jnp.dot(
        leading, trailing, preferred_element_type=jnp.float32, precision=lax.Precision.HIGHEST
    )


def rotate(array, axis, shift):
    size = lax.axis_size(axis)
    return lax.ppermute(array, axis, [(s, (s + shift) % size) for s in range(size)])


def swap(array, axis):
    return lax.ppermute(array, axis, [(0, 1), (1, 0)])


def turn(array):
    return lax.ppermute(array, (XL, CORE), [(0, 0), (1, 2), (2, 1), (3, 3)])


def ordered(mine, other, index):
    first = jnp.where(index == 0, mine, other)
    second = jnp.where(index == 0, other, mine)
    return first, second


def row_panel(block):
    pair = jnp.stack(ordered(block, swap(block, XL), lax.axis_index(XL)))
    copies = jnp.broadcast_to(pair[None], (8,) + pair.shape)
    panel = lax.all_to_all(copies, (Y, XH), 0, 0, tiled=True)
    return panel.reshape((16,) + block.shape)


def column_panel(block):
    place = lax.axis_index(Z)
    found = {0: block}
    for shift in (1, -1, 2, -2):
        found[shift] = rotate(block, Z, shift)
    found[3] = rotate(found[2], Z, 1)
    found[-3] = rotate(found[-2], Z, -1)
    found[4] = rotate(found[2], Z, 2)
    mine = jnp.zeros((8,) + block.shape, block.dtype)
    for shift, piece in found.items():
        mine = lax.dynamic_update_slice(mine, piece[None], ((place - shift) % 8, 0, 0))
    first, second = ordered(mine, swap(mine, CORE), lax.axis_index(CORE))
    return jnp.stack((first, second), axis=1).reshape((16,) + block.shape)


def contract(rows, columns):
    side = rows.shape[1]
    return matmul(rows.transpose(1, 0, 2).reshape(side, -1), columns.reshape(-1, side))


def gradient_panels(gradient):
    piece = gradient.T
    copies = jnp.broadcast_to(piece[None], (8,) + piece.shape)
    along_z = lax.all_to_all(copies, Z, 0, 0, tiled=True)
    own = jnp.stack(ordered(piece, swap(piece, XL), lax.axis_index(XL)))
    for_rows = jnp.tile(own, (8, 1, 1))
    for_columns = jnp.repeat(along_z, 2, axis=0)
    parts = lax.all_to_all(jnp.stack((for_rows, for_columns), axis=1), GY, 0, 0, tiled=True)
    width = piece.shape[1]
    return parts[:, 0].reshape(-1, width), parts[:, 1].reshape(-1, width)


def local(gradient, stat_old):
    side = stat_old.shape[0]
    total = side * 16
    row_block = 2 * lax.axis_index(Z) + lax.axis_index(CORE)
    column_block = 4 * lax.axis_index(Y) + 2 * lax.axis_index(XH) + lax.axis_index(XL)
    eye = jnp.eye(side, dtype=jnp.float32)
    numbers = jnp.arange(16)[:, None, None]

    rows_of, columns_of = gradient_panels(gradient)
    outer = matmul(rows_of.T, columns_of) / rows_of.shape[0]
    stat = 0.9 * turn(stat_old) + outer
    statistic = turn(stat)

    stat_row = row_panel(stat)
    stat_column = column_panel(stat)
    square = contract(stat_row, stat_column)
    row_norm = jnp.sum(stat_row * stat_row)

    square_row = row_panel(square)
    carried = jnp.concatenate((square, jnp.full((8, side), row_norm)), axis=0)
    square_column = column_panel(carried)
    squares = jnp.sum(square_column[:, side, 0])
    divisor = 2.0 * jnp.sqrt(squares / total)
    inverse = 1.0 / divisor
    w_row = (square_row * inverse - 4.5 * stat_row) * inverse + jnp.where(
        numbers == row_block, 3.375, 0.0
    ) * eye
    w_column = (square_column[:, :side] * inverse - 4.5 * stat_column) * inverse + jnp.where(
        numbers == column_block, 3.375, 0.0
    ) * eye
    result = 0.0625 * contract(w_row, w_column) - (0.5390625 * inverse) * stat
    result = result + jnp.where(row_block == column_block, 1.5380859375, 0.0) * eye
    return (statistic, turn(result))


def solution(mesh):
    torus = Mesh(mesh.devices.reshape(8, 2, 4, 2, 2), (Z, XL, Y, XH, CORE))
    placed = (P(GX, GY), P(GX, GY))
    return jax.shard_map(
        local, mesh=torus, in_specs=placed, out_specs=(P(GX, GY), P(GX, GY)), check_vma=False
    )
```

```python
import jax
import jax.numpy as jnp
from jax import lax
from jax.sharding import Mesh
from jax.sharding import PartitionSpec as P


Z, XL, Y, XH, CORE = "gx_0", "gx_1", "gy_0", "gy_1", "gy_2"
GX = (Z, XL)
GY = (Y, XH, CORE)


def matmul(leading, trailing):
    return jnp.dot(
        leading, trailing, preferred_element_type=jnp.float32, precision=lax.Precision.HIGHEST
    )


def rotate(array, axis, shift):
    size = lax.axis_size(axis)
    return lax.ppermute(array, axis, [(s, (s + shift) % size) for s in range(size)])


def swap(array, axis):
    return lax.ppermute(array, axis, [(0, 1), (1, 0)])


def turn(array):
    return lax.ppermute(array, (XL, CORE), [(0, 0), (1, 2), (2, 1), (3, 3)])


def ordered(mine, other, index):
    first = jnp.where(index == 0, mine, other)
    second = jnp.where(index == 0, other, mine)
    return first, second


def row_panel(block):
    copies = jnp.broadcast_to(block[None], (16,) + block.shape)
    return lax.all_to_all(copies, (Y, XH, XL), 0, 0, tiled=True)


def column_panel(block):
    place = lax.axis_index(Z)
    found = {0: block}
    for shift in (2, -2, 1, -1):
        found[shift] = rotate(block, Z, shift)
    found[3] = rotate(found[2], Z, 1)
    found[-3] = rotate(found[-2], Z, -1)
    found[4] = rotate(found[2], Z, 2)
    mine = jnp.zeros((8,) + block.shape, block.dtype)
    for shift, piece in found.items():
        mine = lax.dynamic_update_slice(mine, piece[None], ((place - shift) % 8, 0, 0))
    first, second = ordered(mine, swap(mine, CORE), lax.axis_index(CORE))
    return jnp.stack((first, second), axis=1).reshape((16,) + block.shape)


def contract(rows, columns):
    side = rows.shape[1]
    return matmul(rows.transpose(1, 0, 2).reshape(side, -1), columns.reshape(-1, side))


def gradient_panels(gradient):
    piece = gradient.T
    copies = jnp.broadcast_to(piece[None], (8,) + piece.shape)
    along_z = lax.all_to_all(copies, Z, 0, 0, tiled=True)
    own = jnp.stack(ordered(piece, swap(piece, XL), lax.axis_index(XL)))
    for_rows = jnp.tile(own, (8, 1, 1))
    for_columns = jnp.repeat(along_z, 2, axis=0)
    parts = lax.all_to_all(jnp.stack((for_rows, for_columns), axis=1), GY, 0, 0, tiled=True)
    width = piece.shape[1]
    return parts[:, 0].reshape(-1, width), parts[:, 1].reshape(-1, width)


def local(gradient, stat_old):
    side = stat_old.shape[0]
    total = side * 16
    row_block = 2 * lax.axis_index(Z) + lax.axis_index(CORE)
    column_block = 4 * lax.axis_index(Y) + 2 * lax.axis_index(XH) + lax.axis_index(XL)
    eye = jnp.eye(side, dtype=jnp.float32)
    numbers = jnp.arange(16)[:, None, None]

    rows_of, columns_of = gradient_panels(gradient)
    outer = matmul(rows_of.T, columns_of) / rows_of.shape[0]
    stat = 0.9 * turn(stat_old) + outer

    stat_row = row_panel(stat)
    stat_column = column_panel(stat)
    statistic = turn(stat)
    square = contract(stat_row, stat_column)
    row_norm = jnp.sum(stat_row * stat_row)

    carried = jnp.concatenate((square, jnp.full((8, side), row_norm)), axis=0)
    square_row = row_panel(square)
    square_column = column_panel(carried)
    squares = jnp.sum(square_column[:, side, 0])
    divisor = 2.0 * jnp.sqrt(squares / total)
    inverse = 1.0 / divisor
    w_row = (square_row * inverse - 4.5 * stat_row) * inverse + jnp.where(
        numbers == row_block, 3.375, 0.0
    ) * eye
    w_column = (square_column[:, :side] * inverse - 4.5 * stat_column) * inverse + jnp.where(
        numbers == column_block, 3.375, 0.0
    ) * eye
    result = 0.0625 * contract(w_row, w_column) - (0.5390625 * inverse) * stat
    result = result + jnp.where(row_block == column_block, 1.5380859375, 0.0) * eye
    return (statistic, turn(result))


def solution(mesh):
    torus = Mesh(mesh.devices.reshape(8, 2, 4, 2, 2), (Z, XL, Y, XH, CORE))
    placed = (P(GX, GY), P(GX, GY))
    return jax.shard_map(
        local, mesh=torus, in_specs=placed, out_specs=(P(GX, GY), P(GX, GY)), check_vma=False
    )
```

```python
import jax
import jax.numpy as jnp
from jax import lax
from jax.experimental import pallas as pl
from jax.experimental.pallas import tpu as pltpu
from jax.sharding import Mesh
from jax.sharding import PartitionSpec as P


Z, XL, Y, XH, CORE = "gx_0", "gx_1", "gy_0", "gy_1", "gy_2"
GX = (Z, XL)
GY = (Y, XH, CORE)


def matmul(leading, trailing):
    return jnp.dot(
        leading, trailing, preferred_element_type=jnp.float32, precision=lax.Precision.HIGHEST
    )


def rotate(array, axis, shift):
    size = lax.axis_size(axis)
    return lax.ppermute(array, axis, [(s, (s + shift) % size) for s in range(size)])


def swap(array, axis):
    return lax.ppermute(array, axis, [(0, 1), (1, 0)])


def turn(array):
    return lax.ppermute(array, (XL, CORE), [(0, 0), (1, 2), (2, 1), (3, 3)])


def row_panel(copies):
    return lax.all_to_all(copies, (Y, XH, XL), 0, 0, tiled=True)


def column_pieces(block):
    place = lax.axis_index(Z)
    found = {0: block}
    for shift in (2, -2, 1, -1):
        found[shift] = rotate(block, Z, shift)
    found[3] = rotate(found[2], Z, 1)
    found[-3] = rotate(found[-2], Z, -1)
    found[4] = rotate(found[2], Z, 2)
    mine = jnp.zeros((8,) + block.shape, block.dtype)
    for shift, piece in found.items():
        mine = lax.dynamic_update_slice(mine, piece[None], ((place - shift) % 8, 0, 0))
    return mine, swap(mine, CORE)


def exchange(array):
    places = [(z, x, g, c) for z in range(8) for x in range(2) for g in range(8) for c in range(2)]
    pairs = [
        (((z * 2 + x) * 8 + g) * 2 + c, ((g * 2 + x) * 8 + z) * 2 + c) for z, x, g, c in places
    ]
    return lax.ppermute(array, (Z, XL, Y, XH, CORE), pairs)


def outer_part(gradient):
    piece = gradient.T
    beside = swap(piece, XL)
    moved = exchange(piece)
    at_high = lax.axis_index(XL) == 1
    pair = jnp.stack((jnp.where(at_high, beside, piece), jnp.where(at_high, piece, beside)))
    rows_of = lax.all_to_all(jnp.tile(pair, (8, 1, 1)), GY, 0, 0, tiled=True)
    mine, other = column_pieces(moved)
    core = lax.axis_index(CORE)
    columns_of = jnp.stack(
        (jnp.where(core == 0, mine, other), jnp.where(core == 0, other, mine)), axis=1
    )
    width = piece.shape[1]
    return matmul(rows_of.reshape(-1, width).T, columns_of.reshape(-1, width))


def split(array):
    high = array.astype(jnp.bfloat16)
    return high, (array - high.astype(jnp.float32)).astype(jnp.bfloat16)


def product(left, right):
    left_high, left_low = split(left)
    right_high, right_low = split(right)

    def dot(one, two):
        return jnp.dot(one, two, preferred_element_type=jnp.float32)

    return dot(left_high, right_high) + (dot(left_high, right_low) + dot(left_low, right_high))


def square_kernel(core_ref, row_ref, mine_ref, other_ref, copies_ref, carried_ref):
    core = core_ref[0]
    side = mine_ref.shape[1]
    total = jnp.zeros((side, mine_ref.shape[2]), jnp.float32)
    norms = jnp.zeros((side, side), jnp.float32)
    for place in range(mine_ref.shape[0]):
        first = row_ref[2 * place + core]
        second = row_ref[2 * place + 1 - core]
        total = total + product(
            jnp.concatenate((first, second), axis=1),
            jnp.concatenate((mine_ref[place], other_ref[place]), axis=0),
        )
        norms = norms + first * first + second * second
    for number in range(copies_ref.shape[0]):
        copies_ref[number] = total
    carried_ref[:side] = total
    carried_ref[side:] = jnp.full((carried_ref.shape[0] - side, side), jnp.sum(norms))


def root_kernel(
    index_ref, square_row, stat_row, square_mine, square_other, stat_mine, stat_other, stat, out
):
    core, row_block, column_block = index_ref[0], index_ref[1], index_ref[2]
    places, side = stat_mine.shape[0], stat.shape[0]
    sums = jnp.zeros((8, side), jnp.float32)
    for place in range(places):
        sums = sums + square_mine[place, side : side + 8] + square_other[place, side : side + 8]
    divisor = 2.0 * jnp.sqrt(sums[:1] / (2 * places * side))
    inverse = 1.0 / divisor
    across = lax.broadcasted_iota(jnp.int32, (side, side), 0)
    along = lax.broadcasted_iota(jnp.int32, (side, side), 1)
    eye = jnp.where(across == along, 1.0, 0.0)

    def quadratic(square, plain, on_diagonal):
        scaled = (square * inverse - 4.5 * plain) * inverse
        return scaled + jnp.where(on_diagonal, 3.375, 0.0) * eye

    total = jnp.zeros((side, side), jnp.float32)
    for place in range(places):
        lefts, rights = [], []
        for part, square, plain in ((core, square_mine, stat_mine), (1 - core, square_other, stat_other)):
            number = 2 * place + part
            lefts.append(quadratic(square_row[number], stat_row[number], number == row_block))
            rights.append(quadratic(square[place, :side], plain[place], number == column_block))
        total = total + product(jnp.concatenate(lefts, axis=1), jnp.concatenate(rights, axis=0))
    constant = jnp.where(row_block == column_block, 1.5380859375, 0.0) * eye
    out[...] = 0.0625 * total - (0.5390625 * inverse) * stat[...] + constant


def call(kernel, outs, *operands):
    spaces = [pl.BlockSpec(memory_space=pltpu.SMEM)] + [
        pl.BlockSpec(memory_space=pltpu.VMEM) for _ in operands[1:]
    ]
    return pl.pallas_call(
        kernel,
        out_shape=[jax.ShapeDtypeStruct(shape, jnp.float32) for shape in outs],
        in_specs=spaces,
        out_specs=[pl.BlockSpec(memory_space=pltpu.VMEM) for _ in outs],
    )(*operands)


def local(gradient, stat_old):
    side = stat_old.shape[0]
    core = lax.axis_index(CORE)
    row_block = 2 * lax.axis_index(Z) + core
    column_block = 4 * lax.axis_index(Y) + 2 * lax.axis_index(XH) + lax.axis_index(XL)

    indices = jnp.stack((core, row_block, column_block))

    outer = outer_part(gradient)
    stat_moved = turn(stat_old)
    stat = 0.9 * stat_moved + outer / (gradient.shape[1] * 16)

    stat_row = row_panel(jnp.broadcast_to(stat[None], (16,) + stat.shape))
    stat_mine, stat_other = column_pieces(stat)
    statistic = turn(stat)
    copies, carried = call(
        square_kernel,
        ((16, side, side), (side + 8, side)),
        indices,
        stat_row,
        stat_mine,
        stat_other,
    )
    square_row = row_panel(copies)
    square_mine, square_other = column_pieces(carried)
    (result,) = call(
        root_kernel,
        ((side, side),),
        indices,
        square_row,
        stat_row,
        square_mine,
        square_other,
        stat_mine,
        stat_other,
        stat,
    )
    return (statistic, turn(result))


def solution(mesh):
    torus = Mesh(mesh.devices.reshape(8, 2, 4, 2, 2), (Z, XL, Y, XH, CORE))
    placed = (P(GX, GY), P(GX, GY))
    return jax.shard_map(
        local, mesh=torus, in_specs=placed, out_specs=(P(GX, GY), P(GX, GY)), check_vma=False
    )
```

```python
import jax
import jax.numpy as jnp
from jax import lax
from jax.experimental import pallas as pl
from jax.experimental.pallas import tpu as pltpu
from jax.sharding import Mesh
from jax.sharding import PartitionSpec as P


Z, XL, Y, XH, CORE = "gx_0", "gx_1", "gy_0", "gy_1", "gy_2"
GX = (Z, XL)
GY = (Y, XH, CORE)
VMEM_BYTES = 20 * 1024 * 1024


def matmul(leading, trailing):
    return jnp.dot(
        leading, trailing, preferred_element_type=jnp.float32, precision=lax.Precision.HIGHEST
    )


def rotate(array, axis, shift):
    size = lax.axis_size(axis)
    return lax.ppermute(array, axis, [(s, (s + shift) % size) for s in range(size)])


def swap(array, axis):
    return lax.ppermute(array, axis, [(0, 1), (1, 0)])


def turn(array):
    return lax.ppermute(array, (XL, CORE), [(0, 0), (1, 2), (2, 1), (3, 3)])


def row_panel(copies):
    return lax.all_to_all(copies, (Y, XH, XL), 0, 0, tiled=True)


def column_pieces(block):
    place = lax.axis_index(Z)
    found = {0: block}
    for shift in (2, -2, 1, -1):
        found[shift] = rotate(block, Z, shift)
    found[3] = rotate(found[2], Z, 1)
    found[-3] = rotate(found[-2], Z, -1)
    found[4] = rotate(found[2], Z, 2)
    mine = jnp.zeros((8,) + block.shape, block.dtype)
    for shift, piece in found.items():
        mine = lax.dynamic_update_slice(mine, piece[None], ((place - shift) % 8, 0, 0))
    other = swap(mine, CORE)
    return jnp.concatenate((mine, other), axis=0)


def exchange(array):
    places = [(z, x, g, c) for z in range(8) for x in range(2) for g in range(8) for c in range(2)]
    pairs = [
        (((z * 2 + x) * 8 + g) * 2 + c, ((g * 2 + x) * 8 + z) * 2 + c) for z, x, g, c in places
    ]
    return lax.ppermute(array, (Z, XL, Y, XH, CORE), pairs)


def outer_part(gradient):
    piece = gradient.T
    beside = swap(piece, XL)
    moved = exchange(piece)
    at_high = lax.axis_index(XL) == 1
    pair = jnp.stack((jnp.where(at_high, beside, piece), jnp.where(at_high, piece, beside)))
    rows_of = lax.all_to_all(jnp.tile(pair, (8, 1, 1)), GY, 0, 0, tiled=True)
    pieces = column_pieces(moved)
    mine, other = pieces[:8], pieces[8:]
    core = lax.axis_index(CORE)
    columns_of = jnp.stack(
        (jnp.where(core == 0, mine, other), jnp.where(core == 0, other, mine)), axis=1
    )
    width = piece.shape[1]
    return matmul(rows_of.reshape(-1, width).T, columns_of.reshape(-1, width))


def split(array):
    high = array.astype(jnp.bfloat16)
    return high, (array - high.astype(jnp.float32)).astype(jnp.bfloat16)


def product(left, right):
    left_high, left_low = split(left)
    right_high, right_low = split(right)

    def dot(one, two):
        return jnp.dot(one, two, preferred_element_type=jnp.float32)

    return dot(left_high, right_high) + (dot(left_high, right_low) + dot(left_low, right_high))


def square_kernel(row_ref, column_ref, copies_ref, carried_ref):
    core = lax.axis_index(CORE)
    places, side = column_ref.shape[0] // 2, column_ref.shape[1]
    total = jnp.zeros((side, side), jnp.float32)
    norms = jnp.zeros((side, side), jnp.float32)
    for place in range(places):
        first = row_ref[2 * place + core]
        second = row_ref[2 * place + 1 - core]
        total = total + product(
            jnp.concatenate((first, second), axis=1),
            jnp.concatenate((column_ref[place], column_ref[places + place]), axis=0),
        )
        norms = norms + first * first + second * second
    for number in range(copies_ref.shape[0]):
        copies_ref[number] = total
    carried_ref[:side] = total
    carried_ref[side:] = jnp.full((carried_ref.shape[0] - side, side), jnp.sum(norms))


def root_kernel(
    square_row, stat_row, square_column, stat_column, stat, home, out, kept
):
    core = lax.axis_index(CORE)
    row_block = 2 * lax.axis_index(Z) + core
    column_block = 4 * lax.axis_index(Y) + 2 * lax.axis_index(XH) + lax.axis_index(XL)
    kept[...] = home[...]
    places, side = stat_column.shape[0] // 2, stat.shape[0]
    sums = jnp.zeros((8, side), jnp.float32)
    for place in range(2 * places):
        sums = sums + square_column[place, side : side + 8]
    divisor = 2.0 * jnp.sqrt(sums[:1] / (2 * places * side))
    inverse = 1.0 / divisor
    across = lax.broadcasted_iota(jnp.int32, (side, side), 0)
    along = lax.broadcasted_iota(jnp.int32, (side, side), 1)
    eye = jnp.where(across == along, 1.0, 0.0)

    def quadratic(square, plain, on_diagonal):
        scaled = (square * inverse - 4.5 * plain) * inverse
        return scaled + jnp.where(on_diagonal, 3.375, 0.0) * eye

    total = jnp.zeros((side, side), jnp.float32)
    for place in range(places):
        lefts, rights = [], []
        for part, piece in ((core, place), (1 - core, places + place)):
            number = 2 * place + part
            lefts.append(quadratic(square_row[number], stat_row[number], number == row_block))
            rights.append(quadratic(square_column[piece, :side], stat_column[piece], number == column_block))
        total = total + product(jnp.concatenate(lefts, axis=1), jnp.concatenate(rights, axis=0))
    constant = jnp.where(row_block == column_block, 1.5380859375, 0.0) * eye
    out[...] = 0.0625 * total - (0.5390625 * inverse) * stat[...] + constant


def call(kernel, outs, *operands):
    return pl.pallas_call(
        kernel,
        out_shape=[jax.ShapeDtypeStruct(shape, jnp.float32) for shape in outs],
        in_specs=[pl.BlockSpec(memory_space=pltpu.VMEM) for _ in operands],
        out_specs=[pl.BlockSpec(memory_space=pltpu.VMEM) for _ in outs],
        compiler_params=pltpu.CompilerParams(vmem_limit_bytes=VMEM_BYTES),
    )(*operands)


def local(gradient, stat_old):
    side = stat_old.shape[0]
    outer = outer_part(gradient)
    stat_moved = turn(stat_old)
    stat = 0.9 * stat_moved + outer / (gradient.shape[1] * 16)

    stat_row = row_panel(jnp.broadcast_to(stat[None], (16,) + stat.shape))
    stat_column = column_pieces(stat)
    home = turn(stat)
    copies, carried = call(
        square_kernel,
        ((16, side, side), (side + 8, side)),
        stat_row,
        stat_column,
    )
    square_row = row_panel(copies)
    square_column = column_pieces(carried)
    result, statistic = call(
        root_kernel,
        ((side, side), (side, side)),
        square_row,
        stat_row,
        square_column,
        stat_column,
        stat,
        home,
    )
    return (statistic, turn(result))


def solution(mesh):
    torus = Mesh(mesh.devices.reshape(8, 2, 4, 2, 2), (Z, XL, Y, XH, CORE))
    placed = (P(GX, GY), P(GX, GY))
    return jax.shard_map(
        local, mesh=torus, in_specs=placed, out_specs=(P(GX, GY), P(GX, GY)), check_vma=False
    )
```

```python
import jax
import jax.numpy as jnp
from jax import lax
from jax.experimental import pallas as pl
from jax.experimental.pallas import tpu as pltpu
from jax.sharding import Mesh
from jax.sharding import PartitionSpec as P


Z, XL, Y, XH, CORE = "gx_0", "gx_1", "gy_0", "gy_1", "gy_2"
GX = (Z, XL)
GY = (Y, XH, CORE)
VMEM_BYTES = 20 * 1024 * 1024


def matmul(leading, trailing):
    return jnp.dot(
        leading, trailing, preferred_element_type=jnp.float32, precision=lax.Precision.HIGHEST
    )


def rotate(array, axis, shift):
    size = lax.axis_size(axis)
    return lax.ppermute(array, axis, [(s, (s + shift) % size) for s in range(size)])


def swap(array, axis):
    return lax.ppermute(array, axis, [(0, 1), (1, 0)])


def turn(array):
    return lax.ppermute(array, (XL, CORE), [(0, 0), (1, 2), (2, 1), (3, 3)])


def row_panel(copies):
    return lax.all_to_all(copies, (Y, XH, XL), 0, 0, tiled=True)


def plain_slot(place):
    return place


def column_pieces(block, slot=plain_slot):
    place = lax.axis_index(Z)
    found = {0: block}
    for shift in (2, -2, 1, -1):
        found[shift] = rotate(block, Z, shift)
    found[3] = rotate(found[2], Z, 1)
    found[-3] = rotate(found[-2], Z, -1)
    found[4] = rotate(found[2], Z, 2)
    mine = jnp.zeros((8,) + block.shape, block.dtype)
    for shift, piece in found.items():
        mine = lax.dynamic_update_slice(mine, piece[None], (slot((place - shift) % 8), 0, 0))
    other = swap(mine, CORE)
    return jnp.concatenate((mine, other), axis=0)


OFFSETS = (5, 3, 1, 2, 0, 6, 4, 7)


def origin(away, group):
    packed = sum(offset << (3 * number) for number, offset in enumerate(OFFSETS))
    offset = (packed >> (3 * away)) & 7
    return ((group & 6) + (offset & 6)) & 6 | ((group ^ offset) & 1)


def exchange(array):
    places = [(z, x, g, c) for z in range(8) for x in range(2) for g in range(8) for c in range(2)]
    pairs = [
        (((g * 2 + x) * 8 + origin((z - g) % 8, g)) * 2 + c, ((z * 2 + x) * 8 + g) * 2 + c)
        for z, x, g, c in places
    ]
    return lax.ppermute(array, (Z, XL, Y, XH, CORE), pairs)


def outer_part(gradient):
    piece = gradient.T
    beside = swap(piece, XL)
    moved = exchange(piece)
    at_high = lax.axis_index(XL) == 1
    pair = jnp.stack((jnp.where(at_high, beside, piece), jnp.where(at_high, piece, beside)))
    rows_of = lax.all_to_all(jnp.tile(pair, (8, 1, 1)), GY, 0, 0, tiled=True)
    group = 2 * lax.axis_index(Y) + lax.axis_index(XH)
    pieces = column_pieces(moved, lambda place: origin((place - group) % 8, group))
    mine, other = pieces[:8], pieces[8:]
    core = lax.axis_index(CORE)
    columns_of = jnp.stack(
        (jnp.where(core == 0, mine, other), jnp.where(core == 0, other, mine)), axis=1
    )
    width = piece.shape[1]
    return matmul(rows_of.reshape(-1, width).T, columns_of.reshape(-1, width))


def split(array):
    high = array.astype(jnp.bfloat16)
    return high, (array - high.astype(jnp.float32)).astype(jnp.bfloat16)


def product(left, right):
    left_high, left_low = split(left)
    right_high, right_low = split(right)

    def dot(one, two):
        return jnp.dot(one, two, preferred_element_type=jnp.float32)

    return dot(left_high, right_high) + (dot(left_high, right_low) + dot(left_low, right_high))


def square_kernel(row_ref, column_ref, copies_ref, carried_ref):
    core = lax.axis_index(CORE)
    places, side = column_ref.shape[0] // 2, column_ref.shape[1]
    total = jnp.zeros((side, side), jnp.float32)
    norms = jnp.zeros((side, side), jnp.float32)
    for place in range(places):
        first = row_ref[2 * place + core]
        second = row_ref[2 * place + 1 - core]
        total = total + product(
            jnp.concatenate((first, second), axis=1),
            jnp.concatenate((column_ref[place], column_ref[places + place]), axis=0),
        )
        norms = norms + first * first + second * second
    for number in range(copies_ref.shape[0]):
        copies_ref[number] = total
    carried_ref[:side] = total
    carried_ref[side:] = jnp.full((carried_ref.shape[0] - side, side), jnp.sum(norms))


def root_kernel(
    square_row, stat_row, square_column, stat_column, stat, home, out, kept
):
    core = lax.axis_index(CORE)
    row_block = 2 * lax.axis_index(Z) + core
    column_block = 4 * lax.axis_index(Y) + 2 * lax.axis_index(XH) + lax.axis_index(XL)
    kept[...] = home[...]
    places, side = stat_column.shape[0] // 2, stat.shape[0]
    sums = jnp.zeros((8, side), jnp.float32)
    for place in range(2 * places):
        sums = sums + square_column[place, side : side + 8]
    divisor = 2.0 * jnp.sqrt(sums[:1] / (2 * places * side))
    inverse = 1.0 / divisor
    across = lax.broadcasted_iota(jnp.int32, (side, side), 0)
    along = lax.broadcasted_iota(jnp.int32, (side, side), 1)
    eye = jnp.where(across == along, 1.0, 0.0)

    def quadratic(square, plain, on_diagonal):
        scaled = (square * inverse - 4.5 * plain) * inverse
        return scaled + jnp.where(on_diagonal, 3.375, 0.0) * eye

    total = jnp.zeros((side, side), jnp.float32)
    for place in range(places):
        lefts, rights = [], []
        for part, piece in ((core, place), (1 - core, places + place)):
            number = 2 * place + part
            lefts.append(quadratic(square_row[number], stat_row[number], number == row_block))
            rights.append(quadratic(square_column[piece, :side], stat_column[piece], number == column_block))
        total = total + product(jnp.concatenate(lefts, axis=1), jnp.concatenate(rights, axis=0))
    constant = jnp.where(row_block == column_block, 1.5380859375, 0.0) * eye
    out[...] = 0.0625 * total - (0.5390625 * inverse) * stat[...] + constant


def call(kernel, outs, *operands):
    return pl.pallas_call(
        kernel,
        out_shape=[jax.ShapeDtypeStruct(shape, jnp.float32) for shape in outs],
        in_specs=[pl.BlockSpec(memory_space=pltpu.VMEM) for _ in operands],
        out_specs=[pl.BlockSpec(memory_space=pltpu.VMEM) for _ in outs],
        compiler_params=pltpu.CompilerParams(vmem_limit_bytes=VMEM_BYTES),
    )(*operands)


def local(gradient, stat_old):
    side = stat_old.shape[0]
    outer = outer_part(gradient)
    stat_moved = turn(stat_old)
    stat = 0.9 * stat_moved + outer / (gradient.shape[1] * 16)

    stat_row = row_panel(jnp.broadcast_to(stat[None], (16,) + stat.shape))
    stat_column = column_pieces(stat)
    home = turn(stat)
    copies, carried = call(
        square_kernel,
        ((16, side, side), (side + 8, side)),
        stat_row,
        stat_column,
    )
    square_row = row_panel(copies)
    square_column = column_pieces(carried)
    result, statistic = call(
        root_kernel,
        ((side, side), (side, side)),
        square_row,
        stat_row,
        square_column,
        stat_column,
        stat,
        home,
    )
    return (statistic, turn(result))


def solution(mesh):
    torus = Mesh(mesh.devices.reshape(8, 2, 4, 2, 2), (Z, XL, Y, XH, CORE))
    placed = (P(GX, GY), P(GX, GY))
    return jax.shard_map(
        local, mesh=torus, in_specs=placed, out_specs=(P(GX, GY), P(GX, GY)), check_vma=False
    )
```

```python
import jax
import jax.numpy as jnp
from jax import lax
from jax.experimental import pallas as pl
from jax.experimental.pallas import tpu as pltpu
from jax.sharding import Mesh
from jax.sharding import PartitionSpec as P


Z, XL, Y, XH, CORE = "gx_0", "gx_1", "gy_0", "gy_1", "gy_2"
GX = (Z, XL)
GY = (Y, XH, CORE)
VMEM_BYTES = 20 * 1024 * 1024


def matmul(leading, trailing):
    return jnp.dot(
        leading, trailing, preferred_element_type=jnp.float32, precision=lax.Precision.HIGHEST
    )


def rotate(array, axis, shift):
    size = lax.axis_size(axis)
    return lax.ppermute(array, axis, [(s, (s + shift) % size) for s in range(size)])


def swap(array, axis):
    return lax.ppermute(array, axis, [(0, 1), (1, 0)])


def turn(array):
    return lax.ppermute(array, (XL, CORE), [(0, 0), (1, 2), (2, 1), (3, 3)])


def row_panel(copies):
    return lax.all_to_all(copies, (Y, XH, XL), 0, 0, tiled=True)


def plain_slot(place):
    return place


def column_pieces(block, slot=plain_slot):
    place = lax.axis_index(Z)
    found = {0: block}
    for shift in (2, -2, 1, -1):
        found[shift] = rotate(block, Z, shift)
    found[3] = rotate(found[2], Z, 1)
    found[-3] = rotate(found[-2], Z, -1)
    found[4] = rotate(found[2], Z, 2)
    mine = jnp.zeros((8,) + block.shape, block.dtype)
    for shift, piece in found.items():
        mine = lax.dynamic_update_slice(mine, piece[None], (slot((place - shift) % 8), 0, 0))
    other = swap(mine, CORE)
    return jnp.concatenate((mine, other), axis=0)


OFFSETS = (5, 3, 1, 2, 0, 6, 4, 7)


def origin(away, group):
    packed = sum(offset << (3 * number) for number, offset in enumerate(OFFSETS))
    offset = (packed >> (3 * away)) & 7
    return ((group & 6) + (offset & 6)) & 6 | ((group ^ offset) & 1)


def exchange(array):
    places = [(z, x, g, c) for z in range(8) for x in range(2) for g in range(8) for c in range(2)]
    pairs = [
        (((g * 2 + x) * 8 + origin((z - g) % 8, g)) * 2 + c, ((z * 2 + x) * 8 + g) * 2 + c)
        for z, x, g, c in places
    ]
    return lax.ppermute(array, (Z, XL, Y, XH, CORE), pairs)


def outer_part(gradient):
    piece = gradient.T
    beside = swap(piece, XL)
    moved = exchange(piece)
    at_high = lax.axis_index(XL) == 1
    pair = jnp.stack((jnp.where(at_high, beside, piece), jnp.where(at_high, piece, beside)))
    rows_of = lax.all_to_all(jnp.tile(pair, (8, 1, 1)), GY, 0, 0, tiled=True)
    group = 2 * lax.axis_index(Y) + lax.axis_index(XH)
    pieces = column_pieces(moved, lambda place: origin((place - group) % 8, group))
    mine, other = pieces[:8], pieces[8:]
    core = lax.axis_index(CORE)
    columns_of = jnp.stack(
        (jnp.where(core == 0, mine, other), jnp.where(core == 0, other, mine)), axis=1
    )
    width = piece.shape[1]
    return rows_of.reshape(-1, width), columns_of.reshape(-1, width)


def split(array):
    high = array.astype(jnp.bfloat16)
    return high, (array - high.astype(jnp.float32)).astype(jnp.bfloat16)


def product(left, right):
    left_high, left_low = split(left)
    right_high, right_low = split(right)

    def dot(one, two):
        return jnp.dot(one, two, preferred_element_type=jnp.float32)

    return dot(left_high, right_high) + (dot(left_high, right_low) + dot(left_low, right_high))


def stat_kernel(rows_ref, columns_ref, old_ref, copies_ref, stat_ref):
    outer = matmul(rows_ref[...].T, columns_ref[...])
    total = 0.9 * old_ref[...] + outer / rows_ref.shape[0]
    for number in range(copies_ref.shape[0]):
        copies_ref[number] = total
    stat_ref[...] = total


def square_kernel(row_ref, column_ref, copies_ref, carried_ref):
    core = lax.axis_index(CORE)
    places, side = column_ref.shape[0] // 2, column_ref.shape[1]
    total = jnp.zeros((side, side), jnp.float32)
    norms = jnp.zeros((side, side), jnp.float32)
    for place in range(places):
        first = row_ref[2 * place + core]
        second = row_ref[2 * place + 1 - core]
        total = total + product(
            jnp.concatenate((first, second), axis=1),
            jnp.concatenate((column_ref[place], column_ref[places + place]), axis=0),
        )
        norms = norms + first * first + second * second
    for number in range(copies_ref.shape[0]):
        copies_ref[number] = total
    carried_ref[:side] = total
    carried_ref[side:] = jnp.full((carried_ref.shape[0] - side, side), jnp.sum(norms))


def root_kernel(
    square_row, stat_row, square_column, stat_column, stat, home, out, kept
):
    core = lax.axis_index(CORE)
    row_block = 2 * lax.axis_index(Z) + core
    column_block = 4 * lax.axis_index(Y) + 2 * lax.axis_index(XH) + lax.axis_index(XL)
    kept[...] = home[...]
    places, side = stat_column.shape[0] // 2, stat.shape[0]
    sums = jnp.zeros((8, side), jnp.float32)
    for place in range(2 * places):
        sums = sums + square_column[place, side : side + 8]
    divisor = 2.0 * jnp.sqrt(sums[:1] / (2 * places * side))
    inverse = 1.0 / divisor
    across = lax.broadcasted_iota(jnp.int32, (side, side), 0)
    along = lax.broadcasted_iota(jnp.int32, (side, side), 1)
    eye = jnp.where(across == along, 1.0, 0.0)

    def quadratic(square, plain, on_diagonal):
        scaled = (square * inverse - 4.5 * plain) * inverse
        return scaled + jnp.where(on_diagonal, 3.375, 0.0) * eye

    total = jnp.zeros((side, side), jnp.float32)
    for place in range(places):
        lefts, rights = [], []
        for part, piece in ((core, place), (1 - core, places + place)):
            number = 2 * place + part
            lefts.append(quadratic(square_row[number], stat_row[number], number == row_block))
            rights.append(quadratic(square_column[piece, :side], stat_column[piece], number == column_block))
        total = total + product(jnp.concatenate(lefts, axis=1), jnp.concatenate(rights, axis=0))
    constant = jnp.where(row_block == column_block, 1.5380859375, 0.0) * eye
    out[...] = 0.0625 * total - (0.5390625 * inverse) * stat[...] + constant


def call(kernel, outs, *operands):
    return pl.pallas_call(
        kernel,
        out_shape=[jax.ShapeDtypeStruct(shape, jnp.float32) for shape in outs],
        in_specs=[pl.BlockSpec(memory_space=pltpu.VMEM) for _ in operands],
        out_specs=[pl.BlockSpec(memory_space=pltpu.VMEM) for _ in outs],
        compiler_params=pltpu.CompilerParams(vmem_limit_bytes=VMEM_BYTES),
    )(*operands)


def local(gradient, stat_old):
    side = stat_old.shape[0]
    rows_of, columns_of = outer_part(gradient)
    stat_moved = turn(stat_old)
    copies, stat = call(
        stat_kernel, ((16, side, side), (side, side)), rows_of, columns_of, stat_moved
    )

    stat_row = row_panel(copies)
    stat_column = column_pieces(stat)
    home = turn(stat)
    copies, carried = call(
        square_kernel,
        ((16, side, side), (side + 8, side)),
        stat_row,
        stat_column,
    )
    square_row = row_panel(copies)
    square_column = column_pieces(carried)
    result, statistic = call(
        root_kernel,
        ((side, side), (side, side)),
        square_row,
        stat_row,
        square_column,
        stat_column,
        stat,
        home,
    )
    return (statistic, turn(result))


def solution(mesh):
    torus = Mesh(mesh.devices.reshape(8, 2, 4, 2, 2), (Z, XL, Y, XH, CORE))
    placed = (P(GX, GY), P(GX, GY))
    return jax.shard_map(
        local, mesh=torus, in_specs=placed, out_specs=(P(GX, GY), P(GX, GY)), check_vma=False
    )
```
